32 devices in a mesh: rows: 8 (over y, x, core), grp: 4 (over z).
Axes of the slice: x: 2, y: 2, z: 4, core: 2. Of those that a mesh axis runs over, the one named last changes fastest.
Arguments:
- matrix: bfloat16 [24576, 16384], P(('rows', 'grp')), may hold values from -3000 to 3000, as said below
- keep_mask: int32 [16, 24576], P(None, ('rows', 'grp')), may hold values 0 or 1
Outputs:
- cosine: float32 [16384, 256], P(('rows', 'grp'))
The draws below stay inside these ranges and needn't reach their ends.
Inputs may be any that keep to these rules, and one draw needn't show every extreme that they name: `matrix`: entries are real-valued; row and column magnitudes vary.
All inputs are finite; a program needn't handle non-finite values. No bound on the sum of `keep_mask` on one device may be relied on, other than what follows from the above.
Results may differ from the reference program's by a relative error of at most 0.0003.
Values sent between devices are 32-bit elements; how exact they have to be, the bound alone decides.
A program may use at most 192 MiB of HBM per device.

```python
import math
import jax
import jax.numpy as jnp
from jax import lax

COLS = 16384
BLOCK = 1024
WINDOW = 256
ROW_DEV = 768
NBLK = 16
ROWS_ALL = 24576


def draw_matrix(key, part):
    key_base, key_row, key_col = jax.random.split(jax.random.fold_in(key, 7), 3)
    position = jnp.arange(ROWS_ALL, dtype=jnp.float32) / ROWS_ALL
    row_scale = jnp.exp(position * math.log(3.0) + jax.random.uniform(key_row, (ROWS_ALL,), jnp.float32, 0.0, math.log(10.0)))
    col_scale = jnp.exp(jax.random.uniform(key_col, (COLS,), jnp.float32, 0.0, math.log(10.0)))
    base = jnp.clip(jax.random.normal(key_base, (ROWS_ALL, COLS), jnp.float32), -6.0, 6.0)
    return (base * row_scale[:, None] * col_scale[None, :]).astype(jnp.bfloat16)


def with_ends(array, key, low, top_value):
    shape = array.shape
    place = [jax.random.randint(jax.random.fold_in(key, axis), (), 0, shape[axis]) for axis in range(len(shape))]
    array = array.at[tuple(place)].set(low)
    longest = shape.index(max(shape))
    place[longest] = (place[longest] + 1) % shape[longest]
    return array.at[tuple(place)].set(top_value)


def setup_inputs(seed: int = 0) -> dict:
    arg_keys = jax.random.split(jax.random.key(seed), 3)
    matrix = draw_matrix(jax.random.fold_in(arg_keys[2], 71), 0)
    keep_mask = with_ends((jax.random.randint(arg_keys[1], (NBLK, ROWS_ALL), 0, 2) < 1).astype(jnp.int32), jax.random.fold_in(arg_keys[1], 1), 0, 1)
    return {"matrix": matrix, "keep_mask": keep_mask}


def reference(matrix, keep_mask):
    steps_count = ROWS_ALL // ROW_DEV
    blocks = matrix.reshape(steps_count, ROW_DEV, COLS)
    masks = keep_mask.reshape(NBLK, steps_count, ROW_DEV).transpose(1, 0, 2)

    def accumulate(carry, item):
        square, raw = carry
        block, block_mask = item
        square = square + lax.optimization_barrier(jnp.sum(jnp.square(block.astype(jnp.float32)), axis=0))
        gate = block_mask.T.astype(jnp.bfloat16)
        masked = (block.reshape(ROW_DEV, NBLK, BLOCK) * gate[:, :, None]).reshape(ROW_DEV, COLS)
        raw = raw + jnp.dot(masked.T, masked[:, :WINDOW], preferred_element_type=jnp.float32)
        return ((square, raw), None)
    start = (jnp.zeros((COLS,), jnp.float32), jnp.zeros((COLS, WINDOW), jnp.float32))
    (square, raw), _ = lax.scan(accumulate, start, (blocks, masks))
    inverse = 1.0 / jnp.sqrt(square + 1e-06)
    return raw * inverse[:, None] * inverse[None, :WINDOW]
```

```python
import functools

import jax
import jax.numpy as jnp
from jax import lax
from jax.experimental import pallas as pl
from jax.experimental.pallas import tpu as pltpu
from jax.sharding import PartitionSpec as P

WINDOW = 256
STAT = 8
HEIGHT = WINDOW + STAT
SUB = 256
SLOTS = 3
MESH = pl.DeviceIdType.MESH
PIECES_XYZ = (32, 32, 24, 16, 16)
PIECES_YXZ = (32, 24, 24, 16, 16)
PIECES_Z = (("zxy", 16), ("zyx", 16))
EARLY = 2


class Piece:
    def __init__(self, start, height, order):
        self.start, self.height, self.order = start, height, order


def pieces():
    out, at = [], 0
    for order, height in (
        [("xyz", h) for h in PIECES_XYZ]
        + [("yxz", h) for h in PIECES_YXZ]
        + list(PIECES_Z)
    ):
        out.append((at, height, order))
        at += height
    assert at == HEIGHT
    made = [Piece(*p) for p in out]
    a = len(PIECES_XYZ)
    b = a + len(PIECES_YXZ)
    return made[:a], made[a:b], made[b:]


def phase_copies(order, phase, sizes):
    axis, fixed = order[phase], order[:phase]
    groups = [
        (dx, dy)
        for dx in reversed(range(sizes["x"]))
        for dy in reversed(range(sizes["y"]))
        if not ("x" in fixed and dx) and not ("y" in fixed and dy)
    ]
    kept = [g for g in groups if axis == "z" or g["xy".index(axis)] == 0]
    sent = []
    for d in range(1, sizes[axis]):
        if axis == "z":
            sent.append(kept)
        elif axis == "x":
            sent.append([(d, dy) for _, dy in kept])
        else:
            sent.append([(dx, d) for dx, _ in kept])
    return axis, kept, sent


def kernel(cfg, matrix_ref, keep_ref, out_ref, acc, sib_out, sib_in, mbuf, panel,
           masked, wst, load_sem, sib_send, sib_recv, send_sem, recv_sem, *bufs):
    X, Y, Z, tile, width, step = (
        cfg["x"], cfg["y"], cfg["z"], cfg["tile"], cfg["width"], cfg["step"]
    )
    span = Z * tile
    halves = span // step
    rows = lax.axis_index("rows")
    z = lax.axis_index("grp")
    c = lax.rem(rows, 2)
    x = lax.rem(rows // 2, X)
    y = rows // (2 * X)

    def device(yy, xx, cc, zz):
        return ((yy * X + xx) * 2 + cc, zz)

    def quad(g):
        return lax.rem(y + g[1], Y) * X + lax.rem(x + g[0], X)

    def peer(axis, d):
        if axis == "x":
            return device(y, lax.rem(x + d, X), c, z)
        if axis == "y":
            return device(lax.rem(y + d, Y), x, c, z)
        return device(y, x, c, lax.rem(z + d, Z))

    groups = [(dx, dy) for dx in reversed(range(X)) for dy in reversed(range(Y))]
    steps = []
    for gi, g in enumerate(groups):
        for own in (0, 1):
            for h in range(halves):
                steps.append((gi, g, own, h))

    def base(s):
        _, g, own, h = s
        cc = c if own else 1 - c
        return pl.multiple_of((quad(g) * 2 + cc) * span + h * step, step)

    def load(i):
        return pltpu.make_async_copy(
            matrix_ref.at[:, pl.ds(base(steps[i]), step)],
            mbuf.at[i % SLOTS],
            load_sem.at[i % SLOTS],
        )

    window = pltpu.make_async_copy(
        matrix_ref.at[:, pl.ds(0, WINDOW)],
        mbuf.at[SLOTS - 1, :, pl.ds(0, WINDOW)],
        load_sem.at[SLOTS - 1],
    )
    window.start()
    for i in range(SLOTS - 1):
        load(i).start()

    peers = [device(y, x, 1 - c, z)]
    for axis, n in (("x", X), ("y", Y), ("z", Z)):
        peers += [peer(axis, d) for d in range(1, n)]
    barrier = pltpu.get_barrier_semaphore()
    for p in peers:
        pl.semaphore_signal(barrier, inc=1, device_id=p, device_id_type=MESH)

    window.wait()
    first = mbuf[SLOTS - 1, :, pl.ds(0, WINDOW)].astype(jnp.float32)
    window_sq = jnp.sum(first * first, axis=0, keepdims=True)
    panel[...] = first.T * keep_ref[pl.ds(0, 1), :].astype(jnp.float32)
    extra = (WINDOW + tile - 1) // tile
    wst[...] = jnp.zeros_like(wst)
    for e in range(extra):
        part = window_sq[:, e * tile : min(WINDOW, (e + 1) * tile)]
        for t in range(step // tile):
            wst[1 + e : 2 + e, t * tile : t * tile + part.shape[1]] = part
    load(SLOTS - 1).start()
    pl.semaphore_wait(barrier, len(peers))

    def compute(i, dst):
        load(i).wait()
        block = base(steps[i]) // width
        gate = keep_ref[pl.ds(block, 1), :].astype(jnp.float32)
        masked[...] = (panel[...] * gate).astype(jnp.bfloat16)
        first_row = lax.broadcasted_iota(jnp.int32, (STAT, SUB), 0) == 0

        def body(j, carry):
            at = pl.multiple_of(j * SUB, SUB)
            piece = mbuf[i % SLOTS, :, pl.ds(at, SUB)]
            dst[pl.ds(0, WINDOW), pl.ds(at, SUB)] = jnp.dot(
                masked[...], piece, preferred_element_type=jnp.float32
            )
            wide = piece.astype(jnp.float32)
            sq = jnp.sum(wide * wide, axis=0, keepdims=True)
            dst[pl.ds(WINDOW, STAT), pl.ds(at, SUB)] = jnp.where(
                first_row, sq, wst[:, pl.ds(at, SUB)]
            )
            return carry

        lax.fori_loop(0, step // SUB, body, 0)
        if i + SLOTS < len(steps):
            load(i + SLOTS).start()

    list_a, list_b, list_z = pieces()
    sends = {}
    buf_of = {}
    nsem = 0
    nbuf = 0
    for p in list_a + list_b + list_z:
        for phase in range(3):
            axis, kept, sent = phase_copies(p.order, phase, cfg)
            if not sent:
                buf_of[p, phase] = None
                sends[p, phase] = {}
                continue
            ref = bufs[nbuf]
            nbuf += 1
            buf_of[p, phase] = ref
            done = "z" in p.order[:phase]
            out = {}
            for d in range(1, cfg[axis] if axis != "z" else Z):
                for k, g in enumerate(sent[d - 1]):
                    if axis == "z":
                        to = lax.rem(z + d, Z)
                        cols = pl.ds(pl.multiple_of(to * tile, tile), tile)
                    elif done:
                        cols = pl.ds(pl.multiple_of(z * tile, tile), tile)
                    else:
                        cols = pl.ds(0, span)
                    copy = functools.partial(
                        pltpu.make_async_remote_copy,
                        src_ref=acc.at[quad(g), pl.ds(p.start, p.height), cols],
                        dst_ref=ref.at[d - 1, k],
                        send_sem=send_sem.at[nsem],
                        recv_sem=recv_sem.at[nsem],
                        device_id=peer(axis, d),
                        device_id_type=MESH,
                    )
                    nsem += 1
                    out.setdefault(g, []).append(copy)
            sends[p, phase] = out

    def start(p, phase, g=None):
        for key, copies in sends[p, phase].items():
            if g is None or key == g:
                for copy in copies:
                    copy().start()

    def finish(p, phase):
        axis, kept, sent = phase_copies(p.order, phase, cfg)
        for copies in sends[p, phase].values():
            for copy in copies:
                copy().wait_recv()
        if not sent:
            return
        ref = buf_of[p, phase]
        if "z" in p.order[: phase + 1]:
            cols = pl.ds(pl.multiple_of(z * tile, tile), tile)
        else:
            cols = pl.ds(0, span)
        for k, g in enumerate(kept):
            where = (quad(g), pl.ds(p.start, p.height), cols)
            total = acc[where]
            for d in range(len(sent)):
                total = total + ref[d, k]
            acc[where] = total

    def sibling(gi, h):
        n = gi * halves + h
        return pltpu.make_async_remote_copy(
            src_ref=sib_out.at[n],
            dst_ref=sib_in.at[n],
            send_sem=sib_send.at[n],
            recv_sem=sib_recv.at[n],
            device_id=device(y, x, 1 - c, z),
            device_id_type=MESH,
        )

    early = list_z + [p for pair in zip(list_a[:EARLY], list_b[:EARLY]) for p in pair]
    i = 0
    for gi, g in enumerate(groups):
        for h in range(halves):
            compute(i, sib_out.at[gi * halves + h])
            i += 1
            sibling(gi, h).start()
        q = quad(g)
        for h in range(halves):
            compute(i, acc.at[q, :, pl.ds(h * step, step)])
            i += 1
        for h in range(halves):
            sibling(gi, h).wait_recv()

            def add(j, carry, h=h, gi=gi, q=q):
                at = pl.multiple_of(j * 8, 8)
                acc[q, pl.ds(at, 8), pl.ds(h * step, step)] += sib_in[
                    gi * halves + h, pl.ds(at, 8), :
                ]
                return carry

            lax.fori_loop(0, HEIGHT // 8, add, 0)
        for p in early:
            start(p, 0, g)

    count = len(list_a)
    for t in range(count + 2):
        if EARLY <= t + 1 < count:
            start(list_a[t + 1], 0)
            start(list_b[t + 1], 0)
        if t < count:
            for p in (list_a[t], list_b[t]):
                finish(p, 0)
                start(p, 1)
        if t == 0 or t == 1:
            for p in list_z:
                finish(p, t)
                start(p, t + 1)
        if 1 <= t <= count:
            for p in (list_a[t - 1], list_b[t - 1]):
                finish(p, 1)
                start(p, 2)
        if t == 2:
            for p in list_z:
                finish(p, 2)
        if t >= 2:
            for p in (list_a[t - 2], list_b[t - 2]):
                finish(p, 2)

    mine = acc[y * X + x, :, pl.ds(pl.multiple_of(z * tile, tile), tile)]
    own = 1.0 / jnp.sqrt(mine[WINDOW : WINDOW + 1, :] + 1e-06)
    parts = [
        mine[WINDOW + 1 + e : WINDOW + 2 + e, : min(tile, WINDOW - e * tile)]
        for e in range(extra)
    ]
    win = parts[0] if extra == 1 else jnp.concatenate(parts, axis=1)
    win = 1.0 / jnp.sqrt(win + 1e-06)
    out_ref[...] = (mine[:WINDOW, :] * own).T * win

    for gi in range(len(groups)):
        for h in range(halves):
            sibling(gi, h).wait_send()
    for p in list_a + list_b + list_z:
        for phase in range(3):
            for copies in sends[p, phase].values():
                for copy in copies:
                    copy().wait_send()


def shards(matrix, keep_mask):
    depth, columns = matrix.shape
    blocks = keep_mask.shape[0]
    width = columns // blocks
    outer = lax.axis_size("rows")
    inner = lax.axis_size("grp")
    tile = columns // (outer * inner)
    cfg = {"x": 2, "y": outer // 4, "z": inner, "tile": tile, "width": width}
    span = inner * tile
    step = min(width, span)
    cfg["step"] = step
    quads = cfg["x"] * cfg["y"]
    links = quads * (span // step)
    bufs, nsem = [], 0
    for group in pieces():
        for p in group:
            for phase in range(3):
                axis, kept, sent = phase_copies(p.order, phase, cfg)
                if not sent:
                    continue
                cols = tile if "z" in p.order[: phase + 1] else span
                nsem += len(sent) * len(kept)
                bufs.append(
                    pltpu.VMEM((len(sent), len(kept), p.height, cols), jnp.float32)
                )
    return pl.pallas_call(
        functools.partial(kernel, cfg),
        out_shape=jax.ShapeDtypeStruct((tile, WINDOW), jnp.float32),
        in_specs=[
            pl.BlockSpec(memory_space=pl.ANY),
            pl.BlockSpec(memory_space=pltpu.VMEM),
        ],
        out_specs=pl.BlockSpec(memory_space=pltpu.VMEM),
        scratch_shapes=[
            pltpu.VMEM((quads, HEIGHT, span), jnp.float32),
            pltpu.VMEM((links, HEIGHT, step), jnp.float32),
            pltpu.VMEM((links, HEIGHT, step), jnp.float32),
            pltpu.VMEM((SLOTS, depth, step), jnp.bfloat16),
            pltpu.VMEM((WINDOW, depth), jnp.float32),
            pltpu.VMEM((WINDOW, depth), jnp.bfloat16),
            pltpu.VMEM((STAT, step), jnp.float32),
            pltpu.SemaphoreType.DMA((SLOTS,)),
            pltpu.SemaphoreType.DMA((links,)),
            pltpu.SemaphoreType.DMA((links,)),
            pltpu.SemaphoreType.DMA((nsem,)),
            pltpu.SemaphoreType.DMA((nsem,)),
        ]
        + bufs,
        compiler_params=pltpu.CompilerParams(
            collective_id=0, has_side_effects=True, vmem_limit_bytes=62 * 1024 * 1024
        ),
        cost_estimate=pl.CostEstimate(
            flops=2 * depth * columns * WINDOW,
            bytes_accessed=2 * depth * columns,
            transcendentals=0,
        ),
    )(matrix, keep_mask)


def solution(mesh):
    in_specs = (P(("rows", "grp"), None), P(None, ("rows", "grp")))
    out_specs = P(("rows", "grp"), None)
    return jax.shard_map(shards, mesh=mesh, in_specs=in_specs, out_specs=out_specs, check_vma=False)
```
